512 devices in a mesh: groups: 2 (over y), grid: 32 (over z), row: 2 (over core), rep: 4 (over x).
Axes of the slice: x: 4, y: 2, z: 32, core: 2. Of those that a mesh axis runs over, the one named last changes fastest.
The devices are a block of a 4x8x32 slice.
Arguments:
- tokens: bfloat16 [2048, 4096], P(('groups', 'grid', 'rep'), 'row'), parts along dimension 0, may hold values from -40 to 40
- target_tokens: int32 [2048], P('groups'), parts along dimension 0, may hold values from 0 to 31999
- gate_weight: bfloat16 [4096, 14336], P(('row', 'rep'), 'grid'), may hold values from -0.09375 to 0.09375
- up_weight: bfloat16 [4096, 14336], P(('row', 'rep'), 'grid'), may hold values from -0.09375 to 0.09375
- down_weight: bfloat16 [14336, 4096], P('grid', ('row', 'rep')), may hold values from -0.046875 to 0.046875
- norm_gain: float32 [4096], P('row'), may hold values from 0.5 to 1.5
- vocab_weight: bfloat16 [4096, 32000], P('row', ('grid', 'rep')), may hold values from -6 to 6
Outputs:
- mixed: bfloat16 [2048, 4096], P(('groups', 'grid', 'rep'), 'row'), parts along dimension 0
- logprob: float32 [2048], P(('groups', 'grid', 'rep')), parts along dimension 0
The draws below stay inside these ranges and needn't reach their ends.
There are 2 independent parts, one for each index of `groups`. The reference program is written for one: setup_inputs(seed, part) draws one part's arguments, and reference() takes and returns one part's arrays. A program takes and returns all parts, laid end to end along the dimension named above; an argument that names none is the same for every part. Nothing has to cross between parts.
All inputs are finite; a program needn't handle non-finite values.
Results may differ from the reference program's by a relative error of at most 0.0046.
Values may be sent and summed in bfloat16 or wider, within the bound.
No kernel may reach another device: no remote copies, remote signals or barrier semaphores. Data moves between devices by JAX's collectives and lax.ppermute only.
A program may use at most 64 MiB of HBM per device.

```python
import math
import jax
import jax.numpy as jnp
import numpy as np
from jax import lax

D = 4096
FF = 14336
V = 32000
TOKENS = 1024


def draw_tokens(key, part):
    key_rows = jax.random.fold_in(key, 0)
    key_cols = jax.random.fold_in(key, 1)
    key_base = jax.random.fold_in(key, 2)
    key_pick = jax.random.fold_in(key, 4)
    key_level = jax.random.fold_in(key, 5)
    key_noise = jax.random.fold_in(key, 6)
    key_mix = jax.random.fold_in(key, 7)
    row_scale = jnp.exp(jax.random.uniform(key_rows, (TOKENS, 1), minval=math.log(0.4), maxval=math.log(4.0)))
    column_ramp = jnp.arange(D, dtype=jnp.float32) / D
    column_scale = 0.5 * jnp.exp(math.log(3.0) * column_ramp + jax.random.uniform(key_cols, (D,), minval=-0.2, maxval=0.2))
    base_draw = jnp.clip(jax.random.normal(key_base, (TOKENS, D)), -5.5, 5.5)
    drawn = base_draw * row_scale * column_scale
    aligned_row = jax.random.randint(key_pick, (TOKENS, 1), 0, 12) == 0
    level = jax.random.uniform(key_level, (TOKENS, 1), minval=2.0, maxval=3.0)
    mix_share = jax.random.uniform(key_mix, (TOKENS, 1), minval=0.15, maxval=2.0)
    noise = jnp.clip(jax.random.normal(key_noise, (TOKENS, D)), -5.0, 5.0)
    aligned = level * (1.0 + mix_share * noise)
    return jnp.clip(jnp.where(aligned_row, aligned, drawn), -40.0, 40.0).astype(jnp.bfloat16)


def draw_vocab_weight(key, part):
    key_base, key_scale, key_heavy, key_pair = jax.random.split(key, 4)
    column_ramp = jnp.arange(V, dtype=jnp.float32) / V
    column_scale = (2.5 + column_ramp + jax.random.uniform(key_scale, (V,), minval=-0.3, maxval=0.3)) / math.sqrt(D)
    base_draw = jnp.clip(jax.random.normal(key_base, (D, V)), -5.0, 5.0) * column_scale
    heavy_level = 320.0 / D
    heavy_draw = heavy_level * (1.0 + 0.15 * jnp.clip(jax.random.normal(key_heavy, (D, V)), -4.0, 4.0))
    partner_draw = jnp.roll(heavy_draw, 1, axis=1) + jnp.clip(jax.random.normal(key_pair, (D, V)), -5.0, 5.0) * (1.5 / math.sqrt(D))
    position = jnp.arange(V) % (V // 4)
    base_draw = jnp.where(position == 0, heavy_draw, jnp.where(position == 1, partner_draw, base_draw))
    return jnp.clip(base_draw, -6.0, 6.0).astype(jnp.bfloat16)


def set_ends(drawn, rng, least, high):
    dims = drawn.shape
    spot = [jax.random.randint(jax.random.fold_in(rng, axis), (), 0, dims[axis]) for axis in range(len(dims))]
    drawn = drawn.at[tuple(spot)].set(least)
    longest = dims.index(max(dims))
    spot[longest] = (spot[longest] + 1) % dims[longest]
    return drawn.at[tuple(spot)].set(high)


def steps_of(own_key, extent, cuts, low, high):
    def one(axis_at, blocks):
        heights = jax.random.uniform(jax.random.fold_in(jax.random.fold_in(own_key, 6), axis_at), (blocks,), jnp.float32, low / len(cuts), high / len(cuts))
        return jnp.repeat(jnp.exp(heights), extent[axis_at] // blocks).reshape((-1,) + (1,) * (len(extent) - axis_at - 1))

    loudness = one(*cuts[0])
    for cut in cuts[1:]:
        loudness = loudness * one(*cut)
    return loudness


def cumulative_ranks(amount, skew):
    portions = [(1 << 20) // math.isqrt(rank ** skew) + 1 for rank in range(1, amount + 1)]
    scale = 1 + sum(portions) // (1 << 30)
    return np.cumsum(np.array([max(1, weight // scale) for weight in portions]))


def ranked(stream_key, shape, count, lean):
    table = cumulative_ranks(count, lean)
    pick = jax.random.randint(jax.random.fold_in(stream_key, 1), shape, 0, int(table[count - 1]))
    standing = jnp.searchsorted(jnp.asarray(table, jnp.int32), pick, side="right")
    return jax.random.permutation(jax.random.fold_in(stream_key, 2), count)[standing].astype(jnp.int32)


def scatter_about(key, extent, scale, limit, cuts=(), kind=jnp.bfloat16):
    result = jax.random.normal(key, extent, jnp.float32) * scale
    if len(cuts) > 0:
        result = steps_of(key, extent, cuts, -0.22, 0.18) * result
    return jnp.clip(result, min=-limit, max=limit).astype(kind)


def setup_inputs(seed: int = 0, part: int = 0) -> dict:
    streams_of = jax.random.split(jax.random.key(seed), 8)
    part_keys = jax.random.split(jax.random.fold_in(streams_of[7], part), 8)
    tokens = draw_tokens(jax.random.fold_in(jax.random.fold_in(streams_of[7], part), 71), part)
    target_tokens = set_ends(ranked(part_keys[1], (TOKENS,), V, 2), jax.random.fold_in(part_keys[1], 3), 0, V - 1).astype(jnp.int32)
    gate_weight = scatter_about(streams_of[2], (D, FF), D ** -0.5, 0.09375, ((0, 8), (1, 32)))
    up_weight = scatter_about(streams_of[3], (D, FF), D ** -0.5, 0.09375, ((0, 8), (1, 32)))
    down_weight = scatter_about(streams_of[4], (FF, D), FF ** -0.5, 0.046875, ((0, 32), (1, 8)))
    norm_gain = jnp.clip(1.0 + 0.1 * jax.random.normal(streams_of[5], (D,), jnp.float32), 0.5, 1.5)
    vocab_weight = draw_vocab_weight(jax.random.fold_in(streams_of[7], 71), part)
    return {"tokens": tokens, "target_tokens": target_tokens, "gate_weight": gate_weight, "up_weight": up_weight, "down_weight": down_weight, "norm_gain": norm_gain, "vocab_weight": vocab_weight}


def reference(tokens, target_tokens, gate_weight, up_weight, down_weight, norm_gain, vocab_weight):
    gate_value = jnp.dot(tokens, gate_weight, preferred_element_type=jnp.float32)
    up_value = jnp.dot(tokens, up_weight, preferred_element_type=jnp.float32)
    hidden = (jax.nn.silu(gate_value) * up_value).astype(jnp.bfloat16)
    mixed_full = tokens.astype(jnp.float32) + jnp.dot(hidden, down_weight, preferred_element_type=jnp.float32)
    mixed = mixed_full.astype(jnp.bfloat16)
    held = lax.optimization_barrier(mixed).astype(jnp.float32)
    scale = lax.rsqrt(lax.optimization_barrier(jnp.sum(held * held, axis=1, keepdims=True)) / D + 1e-05)
    normed = (held * scale * norm_gain.astype(jnp.float32)).astype(jnp.bfloat16)
    logits = jnp.dot(normed, vocab_weight, preferred_element_type=jnp.float32)
    row_top = lax.optimization_barrier(jnp.max(logits, axis=1, keepdims=True))
    row_total = lax.optimization_barrier(jnp.sum(jnp.exp(logits - row_top), axis=1))
    picked = jnp.take_along_axis(logits, target_tokens.astype(jnp.int32)[:, None], axis=1)[:, 0]
    logprob = picked - row_top[:, 0] - jnp.log(row_total)
    return (mixed, logprob)
```

```python
import jax
import jax.numpy as jnp
from jax import lax
from jax.sharding import PartitionSpec as P


def parity_groups(size):
    return [list(range(side, size, 2)) for side in (0, 1)]


def swapped_in_pairs(value, axis):
    size = lax.axis_size(axis)
    return lax.ppermute(value, axis, [(i, i ^ 1) for i in range(size)])


def gathered_rows(rows, axis):
    own = lax.all_gather(rows, axis, axis=0, axis_index_groups=parity_groups(lax.axis_size(axis)))
    own = own.reshape(-1, rows.shape[1])
    return own, swapped_in_pairs(own, axis)


def both_halves(part, axis):
    return part + lax.ppermute(part, axis, [(0, 1), (1, 0)])


def hidden_units(rows, weights):
    part = jnp.dot(rows, weights, preferred_element_type=jnp.float32)
    value = both_halves(part, "row")
    gate_value, up_value = jnp.split(value, 2, axis=1)
    return (jax.nn.silu(gate_value) * up_value).astype(jnp.bfloat16)


def projected(hidden, weights):
    out = [jnp.dot(hidden, weights[k], preferred_element_type=jnp.float32) for k in range(weights.shape[0])]
    return jnp.concatenate(out, axis=1)


def row_stats(normed, weights, targets, column_start):
    part = jnp.einsum("tk,rkv->rtv", normed, weights, preferred_element_type=jnp.float32)
    logits = both_halves(part, "row")
    ids = lax.broadcasted_iota(jnp.int32, logits.shape, 0) * logits.shape[2] + lax.broadcasted_iota(
        jnp.int32, logits.shape, 2
    )
    top = jnp.max(logits, axis=(0, 2))
    total = jnp.sum(jnp.exp(logits - top[None, :, None]), axis=(0, 2))
    picked = jnp.sum(
        jnp.where(ids == (targets - column_start)[None, :, None], logits, 0.0), axis=(0, 2)
    )
    return jnp.stack([top, total, picked])


def per_device(tokens, target_tokens, gate_weight, up_weight, down_weight, norm_gain, vocab_weight):
    own_rows, half_width = tokens.shape
    features = half_width * lax.axis_size("row")
    grid = lax.axis_size("grid")
    rep = lax.axis_size("rep")
    side = lax.axis_index("grid") % 2

    gate_up = lax.all_gather(
        jnp.concatenate([gate_weight, up_weight], axis=1), "rep", axis=0, tiled=True
    )
    down = lax.all_gather(down_weight, "rep", axis=0)
    vocab = lax.all_gather(vocab_weight, "rep", axis=0)

    own, other = gathered_rows(tokens, "grid")
    hidden_other = hidden_units(other, gate_up)
    branch_other = projected(hidden_other, down).astype(jnp.bfloat16)
    arrived = swapped_in_pairs(branch_other, "grid")
    hidden_own = hidden_units(own, gate_up)
    branch_own = projected(hidden_own, down)
    pair_sum = (branch_own + arrived.astype(jnp.float32)).astype(jnp.bfloat16)
    tiles = lax.all_to_all(
        pair_sum.reshape(grid // 2, own_rows, half_width),
        "grid",
        0,
        0,
        tiled=True,
        axis_index_groups=parity_groups(grid),
    )
    branch_sum = jnp.sum(tiles.astype(jnp.float32), axis=0)
    mixed = (tokens.astype(jnp.float32) + branch_sum).astype(jnp.bfloat16)
    held = lax.optimization_barrier(mixed).astype(jnp.float32)
    squares = lax.psum(jnp.sum(held * held, axis=1), "row")
    scale = lax.rsqrt(squares / features + 1e-05)
    normed = (held * scale[:, None] * norm_gain[None, :]).astype(jnp.bfloat16)

    normed_own, normed_other = gathered_rows(normed, "grid")
    targets = lax.dynamic_slice_in_dim(
        target_tokens.reshape(grid // 2, 2, rep, own_rows), lax.axis_index("rep"), 1, 2
    )[:, :, 0]
    targets_own = lax.dynamic_slice_in_dim(targets, side, 1, 1).reshape(-1)
    targets_other = lax.dynamic_slice_in_dim(targets, 1 - side, 1, 1).reshape(-1)
    column_start = lax.axis_index("grid") * (vocab.shape[0] * vocab.shape[2])
    stats_own = row_stats(normed_own, vocab, targets_own, column_start)
    stats_other = row_stats(normed_other, vocab, targets_other, column_start)
    pieces = jnp.stack([stats_own, stats_other])
    pieces = jnp.where(side == 0, pieces, pieces[::-1]).reshape(2, 3, grid // 2, own_rows)
    pieces = pieces.transpose(2, 0, 1, 3).reshape(grid, 3 * own_rows)
    found = lax.all_to_all(pieces, "grid", 0, 0, tiled=True).reshape(grid, 3, own_rows)
    top = jnp.max(found[:, 0], axis=0)
    total = jnp.sum(found[:, 1] * jnp.exp(found[:, 0] - top[None]), axis=0)
    logprob = jnp.sum(found[:, 2], axis=0) - top - jnp.log(total)
    return (mixed, logprob)


def solution(mesh):
    in_specs = (
        P(("groups", "grid", "rep"), "row"),
        P("groups"),
        P(("row", "rep"), "grid"),
        P(("row", "rep"), "grid"),
        P("grid", ("row", "rep")),
        P("row"),
        P("row", ("grid", "rep")),
    )
    out_specs = (P(("groups", "grid", "rep"), "row"), P(("groups", "grid", "rep")))
    return jax.shard_map(
        per_device, mesh=mesh, in_specs=in_specs, out_specs=out_specs, check_vma=False
    )
```

```python
import jax
import jax.numpy as jnp
from jax import lax
from jax.sharding import PartitionSpec as P


def parity_groups(size):
    return [list(range(side, size, 2)) for side in (0, 1)]


def swapped_in_pairs(value, axis):
    size = lax.axis_size(axis)
    return lax.ppermute(value, axis, [(i, i ^ 1) for i in range(size)])


def gathered_rows(rows, axis):
    own = lax.all_gather(rows, axis, axis=0, axis_index_groups=parity_groups(lax.axis_size(axis)))
    own = own.reshape(-1, rows.shape[1])
    return own, swapped_in_pairs(own, axis)


def both_halves(part, axis):
    return part + lax.ppermute(part, axis, [(0, 1), (1, 0)])


def hidden_units(rows, blocks, width):
    features = blocks.shape[2]
    part = sum(
        lax.dot_general(
            rows[:, k * features : (k + 1) * features],
            blocks[k, :width],
            (((1,), (1,)), ((), ())),
            preferred_element_type=jnp.float32,
        )
        for k in range(blocks.shape[0])
    )
    value = both_halves(part, "row")
    gate_value, up_value = jnp.split(value, 2, axis=1)
    return (jax.nn.silu(gate_value) * up_value).astype(jnp.bfloat16)


def projected(hidden, blocks, width):
    out = [
        jnp.dot(hidden, blocks[k, width:], preferred_element_type=jnp.float32)
        for k in range(blocks.shape[0])
    ]
    return jnp.concatenate(out, axis=1)


def row_stats(normed, weights, targets, column_start):
    part = jnp.einsum("tk,rkv->rtv", normed, weights, preferred_element_type=jnp.float32)
    logits = both_halves(part, "row")
    ids = lax.broadcasted_iota(jnp.int32, logits.shape, 0) * logits.shape[2] + lax.broadcasted_iota(
        jnp.int32, logits.shape, 2
    )
    top = jnp.max(logits, axis=(0, 2))
    total = jnp.sum(jnp.exp(logits - top[None, :, None]), axis=(0, 2))
    picked = jnp.sum(
        jnp.where(ids == (targets - column_start)[None, :, None], logits, 0.0), axis=(0, 2)
    )
    return jnp.stack([top, total, picked])


def per_device(tokens, target_tokens, gate_weight, up_weight, down_weight, norm_gain, vocab_weight):
    own_rows, half_width = tokens.shape
    features = half_width * lax.axis_size("row")
    grid = lax.axis_size("grid")
    rep = lax.axis_size("rep")
    side = lax.axis_index("grid") % 2

    block = jnp.concatenate([gate_weight.T, up_weight.T, down_weight], axis=0)
    blocks = lax.all_gather(block, "rep", axis=0)
    width = gate_weight.shape[1] + up_weight.shape[1]
    vocab = lax.all_gather(vocab_weight, "rep", axis=0)

    own, other = gathered_rows(tokens, "grid")
    hidden = hidden_units(jnp.concatenate([other, own], axis=0), blocks, width)
    hidden_other, hidden_own = jnp.split(hidden, 2, axis=0)
    branch_other = projected(hidden_other, blocks, width).astype(jnp.bfloat16)
    arrived = swapped_in_pairs(branch_other, "grid")
    branch_own = projected(hidden_own, blocks, width)
    pair_sum = (branch_own + arrived.astype(jnp.float32)).astype(jnp.bfloat16)
    tiles = lax.all_to_all(
        pair_sum.reshape(grid // 2, own_rows, half_width),
        "grid",
        0,
        0,
        tiled=True,
        axis_index_groups=parity_groups(grid),
    )
    branch_sum = jnp.sum(tiles.astype(jnp.float32), axis=0)
    mixed = (tokens.astype(jnp.float32) + branch_sum).astype(jnp.bfloat16)
    held = lax.optimization_barrier(mixed).astype(jnp.float32)
    squares = lax.psum(jnp.sum(held * held, axis=1), "row")
    scale = lax.rsqrt(squares / features + 1e-05)
    normed = (held * scale[:, None] * norm_gain[None, :]).astype(jnp.bfloat16)

    normed_own, normed_other = gathered_rows(normed, "grid")
    targets = lax.dynamic_slice_in_dim(
        target_tokens.reshape(grid // 2, 2, rep, own_rows), lax.axis_index("rep"), 1, 2
    )[:, :, 0]
    targets_own = lax.dynamic_slice_in_dim(targets, side, 1, 1).reshape(-1)
    targets_other = lax.dynamic_slice_in_dim(targets, 1 - side, 1, 1).reshape(-1)
    column_start = lax.axis_index("grid") * (vocab.shape[0] * vocab.shape[2])
    stats_own = row_stats(normed_own, vocab, targets_own, column_start)
    stats_other = row_stats(normed_other, vocab, targets_other, column_start)
    pieces = jnp.stack([stats_own, stats_other])
    pieces = jnp.where(side == 0, pieces, pieces[::-1]).reshape(2, 3, grid // 2, own_rows)
    pieces = pieces.transpose(2, 0, 1, 3).reshape(grid, 3 * own_rows)
    found = lax.all_to_all(pieces, "grid", 0, 0, tiled=True).reshape(grid, 3, own_rows)
    top = jnp.max(found[:, 0], axis=0)
    total = jnp.sum(found[:, 1] * jnp.exp(found[:, 0] - top[None]), axis=0)
    logprob = jnp.sum(found[:, 2], axis=0) - top - jnp.log(total)
    return (mixed, logprob)


def solution(mesh):
    in_specs = (
        P(("groups", "grid", "rep"), "row"),
        P("groups"),
        P(("row", "rep"), "grid"),
        P(("row", "rep"), "grid"),
        P("grid", ("row", "rep")),
        P("row"),
        P("row", ("grid", "rep")),
    )
    out_specs = (P(("groups", "grid", "rep"), "row"), P(("groups", "grid", "rep")))
    return jax.shard_map(
        per_device, mesh=mesh, in_specs=in_specs, out_specs=out_specs, check_vma=False
    )
```

```python
import jax
import jax.numpy as jnp
from jax import lax
from jax.sharding import PartitionSpec as P

GATE_UP_REACH = 0.09375
DOWN_REACH = 0.046875


def parity_groups(size):
    return [list(range(side, size, 2)) for side in (0, 1)]


def swapped_in_pairs(value, axis):
    size = lax.axis_size(axis)
    return lax.ppermute(value, axis, [(i, i ^ 1) for i in range(size)])


def gathered_rows(rows, axis):
    own = lax.all_gather(rows, axis, axis=0, axis_index_groups=parity_groups(lax.axis_size(axis)))
    own = own.reshape(-1, rows.shape[1])
    return own, swapped_in_pairs(own, axis)


def both_halves(part, axis):
    return part + lax.ppermute(part, axis, [(0, 1), (1, 0)])


def hidden_units(rows, blocks, width):
    features = blocks.shape[2]
    part = sum(
        lax.dot_general(
            rows[:, k * features : (k + 1) * features],
            blocks[k, :width],
            (((1,), (1,)), ((), ())),
            preferred_element_type=jnp.float32,
        )
        for k in range(blocks.shape[0])
    )
    value = both_halves(part, "row")
    gate_value, up_value = jnp.split(value, 2, axis=1)
    return (jax.nn.silu(gate_value) * up_value).astype(jnp.bfloat16)


def projected(hidden, blocks, width):
    out = [
        jnp.dot(hidden, blocks[k, width:], preferred_element_type=jnp.float32)
        for k in range(blocks.shape[0])
    ]
    return jnp.concatenate(out, axis=1)


def row_stats(normed, weights, targets, column_start):
    part = jnp.einsum("tk,rkv->rtv", normed, weights, preferred_element_type=jnp.float32)
    logits = both_halves(part, "row")
    ids = lax.broadcasted_iota(jnp.int32, logits.shape, 0) * logits.shape[2] + lax.broadcasted_iota(
        jnp.int32, logits.shape, 2
    )
    top = jnp.max(logits, axis=(0, 2))
    total = jnp.sum(jnp.exp(logits - top[None, :, None]), axis=(0, 2))
    picked = jnp.sum(
        jnp.where(ids == (targets - column_start)[None, :, None], logits, 0.0), axis=(0, 2)
    )
    return jnp.stack([top, total, picked])


def per_device(tokens, target_tokens, gate_weight, up_weight, down_weight, norm_gain, vocab_weight):
    own_rows, half_width = tokens.shape
    features = half_width * lax.axis_size("row")
    grid = lax.axis_size("grid")
    rep = lax.axis_size("rep")
    side = lax.axis_index("grid") % 2

    block = jnp.concatenate([gate_weight.T, up_weight.T, down_weight], axis=0)
    blocks = lax.all_gather(block, "rep", axis=0)
    width = gate_weight.shape[1] + up_weight.shape[1]
    vocab = lax.all_gather(vocab_weight, "rep", axis=0)

    own, other = gathered_rows(tokens, "grid")
    rows = jnp.concatenate([other, own], axis=0)
    length = lax.psum(jnp.sum(jnp.abs(rows.astype(jnp.float32)), axis=1), "row")
    units = down_weight.shape[0] * grid
    reach = jnp.maximum(jnp.square(GATE_UP_REACH * length) * (DOWN_REACH * units), 1e-20) / 30000.0
    share = (1.0 / reach)[:, None]
    half = own.shape[0]

    hidden = hidden_units(rows, blocks, width)
    branch_other = (projected(hidden[:half], blocks, width) * share[:half]).astype(jnp.float16)
    arrived = swapped_in_pairs(branch_other, "grid")
    branch_own = projected(hidden[half:], blocks, width) * share[half:]
    pair_sum = (branch_own + arrived.astype(jnp.float32)).astype(jnp.float16)
    branch = lax.psum(pair_sum, "grid", axis_index_groups=parity_groups(grid))
    mixed_own = (own.astype(jnp.float32) + branch.astype(jnp.float32) * reach[half:, None]).astype(
        jnp.bfloat16
    )
    mixed = lax.dynamic_slice_in_dim(mixed_own, lax.axis_index("grid") // 2 * own_rows, own_rows, 0)
    held = lax.optimization_barrier(mixed_own).astype(jnp.float32)
    squares = lax.psum(jnp.sum(held * held, axis=1), "row")
    scale = lax.rsqrt(squares / features + 1e-05)
    normed_own = (held * scale[:, None] * norm_gain[None, :]).astype(jnp.bfloat16)
    normed_other = swapped_in_pairs(normed_own, "grid")
    targets = lax.dynamic_slice_in_dim(
        target_tokens.reshape(grid // 2, 2, rep, own_rows), lax.axis_index("rep"), 1, 2
    )[:, :, 0]
    targets_own = lax.dynamic_slice_in_dim(targets, side, 1, 1).reshape(-1)
    targets_other = lax.dynamic_slice_in_dim(targets, 1 - side, 1, 1).reshape(-1)
    column_start = lax.axis_index("grid") * (vocab.shape[0] * vocab.shape[2])
    stats_own = row_stats(normed_own, vocab, targets_own, column_start)
    stats_other = row_stats(normed_other, vocab, targets_other, column_start)
    pieces = jnp.stack([stats_own, stats_other])
    pieces = jnp.where(side == 0, pieces, pieces[::-1]).reshape(2, 3, grid // 2, own_rows)
    pieces = pieces.transpose(2, 0, 1, 3).reshape(grid, 3 * own_rows)
    found = lax.all_to_all(pieces, "grid", 0, 0, tiled=True).reshape(grid, 3, own_rows)
    top = jnp.max(found[:, 0], axis=0)
    total = jnp.sum(found[:, 1] * jnp.exp(found[:, 0] - top[None]), axis=0)
    logprob = jnp.sum(found[:, 2], axis=0) - top - jnp.log(total)
    return (mixed, logprob)


def solution(mesh):
    in_specs = (
        P(("groups", "grid", "rep"), "row"),
        P("groups"),
        P(("row", "rep"), "grid"),
        P(("row", "rep"), "grid"),
        P("grid", ("row", "rep")),
        P("row"),
        P("row", ("grid", "rep")),
    )
    out_specs = (P(("groups", "grid", "rep"), "row"), P(("groups", "grid", "rep")))
    return jax.shard_map(
        per_device, mesh=mesh, in_specs=in_specs, out_specs=out_specs, check_vma=False
    )
```

```python
import jax
import jax.numpy as jnp
from jax import lax
from jax.sharding import PartitionSpec as P

GATE_UP_REACH = 0.09375
DOWN_REACH = 0.046875


def parity_groups(size):
    return [list(range(side, size, 2)) for side in (0, 1)]


def swapped_in_pairs(value, axis):
    size = lax.axis_size(axis)
    return lax.ppermute(value, axis, [(i, i ^ 1) for i in range(size)])


def gathered_rows(rows, axis):
    own = lax.all_gather(rows, axis, axis=0, axis_index_groups=parity_groups(lax.axis_size(axis)))
    own = own.reshape(-1, rows.shape[1])
    return own, swapped_in_pairs(own, axis)


def sent_to_all(value, axis):
    peers = lax.axis_size(axis)
    return lax.all_to_all(
        jnp.broadcast_to(value[None], (peers, *value.shape)), axis, 0, 0, tiled=True
    )


def both_halves(part, axis):
    return part + lax.ppermute(part, axis, [(0, 1), (1, 0)])


def hidden_units(rows, blocks, width):
    features = blocks.shape[2]
    part = sum(
        lax.dot_general(
            rows[:, k * features : (k + 1) * features],
            blocks[k, :width],
            (((1,), (1,)), ((), ())),
            preferred_element_type=jnp.float32,
        )
        for k in range(blocks.shape[0])
    )
    value = both_halves(part, "row")
    gate_value, up_value = jnp.split(value, 2, axis=1)
    return (jax.nn.silu(gate_value) * up_value).astype(jnp.bfloat16)


def projected(hidden, blocks, width):
    out = [
        jnp.dot(hidden, blocks[k, width:], preferred_element_type=jnp.float32)
        for k in range(blocks.shape[0])
    ]
    return jnp.concatenate(out, axis=1)


def row_stats(normed, weights, targets, column_start):
    part = jnp.einsum("tk,rkv->rtv", normed, weights, preferred_element_type=jnp.float32)
    logits = both_halves(part, "row")
    ids = lax.broadcasted_iota(jnp.int32, logits.shape, 0) * logits.shape[2] + lax.broadcasted_iota(
        jnp.int32, logits.shape, 2
    )
    top = jnp.max(logits, axis=(0, 2))
    total = jnp.sum(jnp.exp(logits - top[None, :, None]), axis=(0, 2))
    picked = jnp.sum(
        jnp.where(ids == (targets - column_start)[None, :, None], logits, 0.0), axis=(0, 2)
    )
    return jnp.stack([top, total, picked])


def per_device(tokens, target_tokens, gate_weight, up_weight, down_weight, norm_gain, vocab_weight):
    own_rows, half_width = tokens.shape
    features = half_width * lax.axis_size("row")
    grid = lax.axis_size("grid")
    rep = lax.axis_size("rep")
    side = lax.axis_index("grid") % 2

    block = jnp.concatenate([gate_weight.T, up_weight.T, down_weight], axis=0)
    blocks = sent_to_all(block, "rep")
    width = gate_weight.shape[1] + up_weight.shape[1]
    vocab = sent_to_all(vocab_weight, "rep")

    own, other = gathered_rows(tokens, "grid")
    rows = jnp.concatenate([other, own], axis=0)
    length = lax.psum(jnp.sum(jnp.abs(rows.astype(jnp.float32)), axis=1), "row")
    units = down_weight.shape[0] * grid
    reach = jnp.maximum(jnp.square(GATE_UP_REACH * length) * (DOWN_REACH * units), 1e-20) / 30000.0
    share = (1.0 / reach)[:, None]
    half = own.shape[0]

    hidden = hidden_units(rows, blocks, width)
    branch_other = (projected(hidden[:half], blocks, width) * share[:half]).astype(jnp.float16)
    arrived = swapped_in_pairs(branch_other, "grid")
    branch_own = projected(hidden[half:], blocks, width) * share[half:]
    pair_sum = (branch_own + arrived.astype(jnp.float32)).astype(jnp.float16)
    branch = lax.psum(pair_sum, "grid", axis_index_groups=parity_groups(grid))
    mixed_own = (own.astype(jnp.float32) + branch.astype(jnp.float32) * reach[half:, None]).astype(
        jnp.bfloat16
    )
    mixed = lax.dynamic_slice_in_dim(mixed_own, lax.axis_index("grid") // 2 * own_rows, own_rows, 0)
    held = lax.optimization_barrier(mixed_own).astype(jnp.float32)
    squares = lax.psum(jnp.sum(held * held, axis=1), "row")
    scale = lax.rsqrt(squares / features + 1e-05)
    normed_own = (held * scale[:, None] * norm_gain[None, :]).astype(jnp.bfloat16)
    normed_other = swapped_in_pairs(normed_own, "grid")
    targets = lax.dynamic_slice_in_dim(
        target_tokens.reshape(grid // 2, 2, rep, own_rows), lax.axis_index("rep"), 1, 2
    )[:, :, 0]
    targets_own = lax.dynamic_slice_in_dim(targets, side, 1, 1).reshape(-1)
    targets_other = lax.dynamic_slice_in_dim(targets, 1 - side, 1, 1).reshape(-1)
    column_start = lax.axis_index("grid") * (vocab.shape[0] * vocab.shape[2])
    stats_own = row_stats(normed_own, vocab, targets_own, column_start)
    stats_other = row_stats(normed_other, vocab, targets_other, column_start)
    pieces = jnp.stack([stats_own, stats_other])
    pieces = jnp.where(side == 0, pieces, pieces[::-1]).reshape(2, 3, grid // 2, own_rows)
    pieces = pieces.transpose(2, 0, 1, 3).reshape(grid, 3 * own_rows)
    found = lax.all_to_all(pieces, "grid", 0, 0, tiled=True).reshape(grid, 3, own_rows)
    top = jnp.max(found[:, 0], axis=0)
    total = jnp.sum(found[:, 1] * jnp.exp(found[:, 0] - top[None]), axis=0)
    logprob = jnp.sum(found[:, 2], axis=0) - top - jnp.log(total)
    return (mixed, logprob)


def solution(mesh):
    in_specs = (
        P(("groups", "grid", "rep"), "row"),
        P("groups"),
        P(("row", "rep"), "grid"),
        P(("row", "rep"), "grid"),
        P("grid", ("row", "rep")),
        P("row"),
        P("row", ("grid", "rep")),
    )
    out_specs = (P(("groups", "grid", "rep"), "row"), P(("groups", "grid", "rep")))
    return jax.shard_map(
        per_device, mesh=mesh, in_specs=in_specs, out_specs=out_specs, check_vma=False
    )
```

```python
import jax
import jax.numpy as jnp
from jax import lax
from jax.sharding import PartitionSpec as P

GATE_UP_REACH = 0.09375
DOWN_REACH = 0.046875


def parity_groups(size):
    return [list(range(side, size, 2)) for side in (0, 1)]


def swapped_in_pairs(value, axis):
    size = lax.axis_size(axis)
    return lax.ppermute(value, axis, [(i, i ^ 1) for i in range(size)])


def sent_to_all(value, axis):
    peers = lax.axis_size(axis)
    return lax.all_to_all(
        jnp.broadcast_to(value[None], (peers, *value.shape)), axis, 0, 0, tiled=True
    )


def shifted(value, axis, step):
    size = lax.axis_size(axis)
    return lax.ppermute(value, axis, [(i, (i + step) % size) for i in range(size)])


def placed(parts, axis, size):
    out = jnp.broadcast_to(parts[0][None], (size, *parts[0].shape))
    for step, value, first_row in parts[1:]:
        place = lax.rem(lax.axis_index(axis) + (step + size), size)
        out = lax.dynamic_update_slice(out, value[None], (place, first_row, 0))
    return out


def both_halves(part, axis):
    return part + lax.ppermute(part, axis, [(0, 1), (1, 0)])


def hidden_units(rows, blocks, width):
    features = blocks.shape[2]
    part = sum(
        lax.dot_general(
            rows[:, k * features : (k + 1) * features],
            blocks[k, :width],
            (((1,), (1,)), ((), ())),
            preferred_element_type=jnp.float32,
        )
        for k in range(blocks.shape[0])
    )
    value = both_halves(part, "row")
    gate_value, up_value = jnp.split(value, 2, axis=1)
    return (jax.nn.silu(gate_value) * up_value).astype(jnp.bfloat16)


def projected(hidden, blocks, width):
    out = [
        jnp.dot(hidden, blocks[k, width:], preferred_element_type=jnp.float32)
        for k in range(blocks.shape[0])
    ]
    return jnp.concatenate(out, axis=1)


def row_stats(normed, weights, targets, column_start):
    part = jnp.einsum("tk,rkv->rtv", normed, weights, preferred_element_type=jnp.float32)
    logits = both_halves(part, "row")
    ids = lax.broadcasted_iota(jnp.int32, logits.shape, 0) * logits.shape[2] + lax.broadcasted_iota(
        jnp.int32, logits.shape, 2
    )
    top = jnp.max(logits, axis=(0, 2))
    total = jnp.sum(jnp.exp(logits - top[None, :, None]), axis=(0, 2))
    picked = jnp.sum(
        jnp.where(ids == (targets - column_start)[None, :, None], logits, 0.0), axis=(0, 2)
    )
    return jnp.stack([top, total, picked])


def device_step(tokens, target_tokens, gate_weight, up_weight, down_weight, norm_gain, vocab_weight):
    own_rows, half_width = tokens.shape
    features = half_width * lax.axis_size("row")
    grid = lax.axis_size("grid")
    rep = lax.axis_size("rep")
    side = lax.rem(lax.axis_index("grid"), 2)

    block = jnp.concatenate([gate_weight.T, up_weight.T, down_weight], axis=0)
    after = shifted(block, "rep", -1)
    before = shifted(block, "rep", 1)
    width = gate_weight.shape[1] + up_weight.shape[1]

    own = lax.all_gather(tokens, "grid", axis=0, axis_index_groups=parity_groups(grid))
    own = own.reshape(-1, half_width)
    own, after_held, before_held = lax.optimization_barrier((own, after, before))
    middle = block.shape[0] // 2
    far_first = shifted(after_held[:middle], "rep", -1)
    far_last = shifted(before_held[middle:], "rep", 1)
    other = swapped_in_pairs(own, "grid")
    vocab = sent_to_all(vocab_weight, "rep")
    blocks = placed(
        [block, (1, after_held, 0), (-1, before_held, 0), (2, far_first, 0), (2, far_last, middle)],
        "rep",
        rep,
    )
    rows = jnp.concatenate([other, own], axis=0)
    length = lax.psum(jnp.sum(jnp.abs(rows.astype(jnp.float32)), axis=1), "row")
    units = down_weight.shape[0] * grid
    reach = jnp.maximum(jnp.square(GATE_UP_REACH * length) * (DOWN_REACH * units), 1e-20) / 30000.0
    share = (1.0 / reach)[:, None]
    half = own.shape[0]

    hidden = hidden_units(rows, blocks, width)
    branch_other = (projected(hidden[:half], blocks, width) * share[:half]).astype(jnp.float16)
    arrived = swapped_in_pairs(branch_other, "grid")
    branch_own = projected(hidden[half:], blocks, width) * share[half:]
    pair_sum = (branch_own + arrived.astype(jnp.float32)).astype(jnp.float16)
    branch = lax.psum(pair_sum, "grid", axis_index_groups=parity_groups(grid))
    mixed_own = (own.astype(jnp.float32) + branch.astype(jnp.float32) * reach[half:, None]).astype(
        jnp.bfloat16
    )
    mixed = lax.dynamic_slice_in_dim(mixed_own, lax.div(lax.axis_index("grid"), 2) * own_rows, own_rows, 0)
    held = lax.optimization_barrier(mixed_own).astype(jnp.float32)
    squares = lax.psum(jnp.sum(held * held, axis=1), "row")
    scale = lax.rsqrt(squares / features + 1e-05)
    normed_own = (held * scale[:, None] * norm_gain[None, :]).astype(jnp.bfloat16)
    normed_other = swapped_in_pairs(normed_own, "grid")
    targets = lax.dynamic_slice_in_dim(
        target_tokens.reshape(grid // 2, 2, rep, own_rows), lax.axis_index("rep"), 1, 2
    )[:, :, 0]
    targets_own = lax.dynamic_slice_in_dim(targets, side, 1, 1).reshape(-1)
    targets_other = lax.dynamic_slice_in_dim(targets, 1 - side, 1, 1).reshape(-1)
    column_start = lax.axis_index("grid") * (vocab.shape[0] * vocab.shape[2])
    stats_own = row_stats(normed_own, vocab, targets_own, column_start)
    stats_other = row_stats(normed_other, vocab, targets_other, column_start)
    pieces = jnp.stack([stats_own, stats_other])
    pieces = jnp.where(side == 0, pieces, pieces[::-1]).reshape(2, 3, grid // 2, own_rows)
    pieces = pieces.transpose(2, 0, 1, 3).reshape(grid, 3 * own_rows)
    found = lax.all_to_all(pieces, "grid", 0, 0, tiled=True).reshape(grid, 3, own_rows)
    top = jnp.max(found[:, 0], axis=0)
    total = jnp.sum(found[:, 1] * jnp.exp(found[:, 0] - top[None]), axis=0)
    logprob = jnp.sum(found[:, 2], axis=0) - top - jnp.log(total)
    return (mixed, logprob)


def solution(mesh):
    in_specs = (
        P(("groups", "grid", "rep"), "row"),
        P("groups"),
        P(("row", "rep"), "grid"),
        P(("row", "rep"), "grid"),
        P("grid", ("row", "rep")),
        P("row"),
        P("row", ("grid", "rep")),
    )
    out_specs = (P(("groups", "grid", "rep"), "row"), P(("groups", "grid", "rep")))
    return jax.shard_map(
        device_step, mesh=mesh, in_specs=in_specs, out_specs=out_specs, check_vma=False
    )
```

```python
import jax
import jax.numpy as jnp
from jax import lax
from jax.sharding import PartitionSpec as P

GATE_UP_REACH = 0.09375
DOWN_REACH = 0.046875


def parity_groups(size):
    return [list(range(side, size, 2)) for side in (0, 1)]


def swapped_in_pairs(value, axis):
    size = lax.axis_size(axis)
    return lax.ppermute(value, axis, [(i, i ^ 1) for i in range(size)])


def sent_to_all(value, axis):
    peers = lax.axis_size(axis)
    return lax.all_to_all(
        jnp.broadcast_to(value[None], (peers, *value.shape)), axis, 0, 0, tiled=True
    )


def shifted(value, axis, step):
    size = lax.axis_size(axis)
    return lax.ppermute(value, axis, [(i, (i + step) % size) for i in range(size)])


def placed(parts, axis, size):
    out = jnp.broadcast_to(parts[0][None], (size, *parts[0].shape))
    for step, value, first_row in parts[1:]:
        place = lax.rem(lax.axis_index(axis) + (step + size), size)
        out = lax.dynamic_update_slice(out, value[None], (place, first_row, 0))
    return out


def both_halves(part, axis):
    return part + lax.ppermute(part, axis, [(0, 1), (1, 0)])


def hidden_units(rows, blocks, width):
    features = blocks.shape[2]
    part = sum(
        lax.dot_general(
            rows[:, k * features : (k + 1) * features],
            blocks[k, :width],
            (((1,), (1,)), ((), ())),
            preferred_element_type=jnp.float32,
        )
        for k in range(blocks.shape[0])
    )
    value = both_halves(part, "row")
    gate_value, up_value = jnp.split(value, 2, axis=1)
    return (jax.nn.silu(gate_value) * up_value).astype(jnp.bfloat16)


def projected(hidden, blocks, width):
    out = [
        jnp.dot(hidden, blocks[k, width:], preferred_element_type=jnp.float32)
        for k in range(blocks.shape[0])
    ]
    return jnp.concatenate(out, axis=1)


def row_stats(normed, weights, targets, column_start):
    part = jnp.einsum("tk,rkv->rtv", normed, weights, preferred_element_type=jnp.float32)
    logits = both_halves(part, "row")
    ids = lax.broadcasted_iota(jnp.int32, logits.shape, 0) * logits.shape[2] + lax.broadcasted_iota(
        jnp.int32, logits.shape, 2
    )
    top = jnp.max(logits, axis=(0, 2))
    total = jnp.sum(jnp.exp(logits - top[None, :, None]), axis=(0, 2))
    picked = jnp.sum(
        jnp.where(ids == (targets - column_start)[None, :, None], logits, 0.0), axis=(0, 2)
    )
    return jnp.stack([top, total, picked])


def device_step(tokens, target_tokens, gate_weight, up_weight, down_weight, norm_gain, vocab_weight):
    own_rows, half_width = tokens.shape
    features = half_width * lax.axis_size("row")
    grid = lax.axis_size("grid")
    rep = lax.axis_size("rep")
    side = lax.rem(lax.axis_index("grid"), 2)

    block = jnp.concatenate([gate_weight.T, up_weight.T, down_weight], axis=0)
    after = shifted(block, "rep", -1)
    before = shifted(block, "rep", 1)
    width = gate_weight.shape[1] + up_weight.shape[1]

    own = lax.all_gather(tokens, "grid", axis=0, axis_index_groups=parity_groups(grid))
    own = own.reshape(-1, half_width)
    own, after_held, before_held = lax.optimization_barrier((own, after, before))
    middle = block.shape[0] // 2
    far_first = shifted(after_held[:middle], "rep", -1)
    far_last = shifted(before_held[middle:], "rep", 1)
    other = swapped_in_pairs(own, "grid")
    vocab = sent_to_all(vocab_weight, "rep")
    blocks = placed(
        [block, (1, after_held, 0), (-1, before_held, 0), (2, far_first, 0), (2, far_last, middle)],
        "rep",
        rep,
    )
    rows = jnp.concatenate([other, own], axis=0)
    length = lax.psum(jnp.sum(jnp.abs(rows.astype(jnp.float32)), axis=1), "row")
    units = down_weight.shape[0] * grid
    reach = jnp.maximum(jnp.square(GATE_UP_REACH * length) * (DOWN_REACH * units), 1e-20) / 30000.0
    share = (1.0 / reach)[:, None]
    half = own.shape[0]

    hidden = hidden_units(rows, blocks, width)
    branch_other = (projected(hidden[:half], blocks, width) * share[:half]).astype(jnp.float16)
    arrived = swapped_in_pairs(branch_other, "grid")
    branch_own = projected(hidden[half:], blocks, width) * share[half:]
    pair_sum = (branch_own + arrived.astype(jnp.float32)).astype(jnp.float16)
    branch = lax.psum(pair_sum, "grid", axis_index_groups=parity_groups(grid))
    mixed_own = (own.astype(jnp.float32) + branch.astype(jnp.float32) * reach[half:, None]).astype(
        jnp.bfloat16
    )
    mixed = lax.dynamic_slice_in_dim(mixed_own, lax.div(lax.axis_index("grid"), 2) * own_rows, own_rows, 0)
    held = lax.optimization_barrier(mixed_own)
    held_other = swapped_in_pairs(held, "grid")
    squares = lax.psum(jnp.sum(jnp.square(held.astype(jnp.float32)), axis=1), "row")
    scale = lax.rsqrt(squares / features + 1e-05)
    scale_other = swapped_in_pairs(scale, "grid")
    normed_own, normed_other = (
        (rows.astype(jnp.float32) * factor[:, None] * norm_gain[None, :]).astype(jnp.bfloat16)
        for rows, factor in ((held, scale), (held_other, scale_other))
    )
    targets = lax.dynamic_slice_in_dim(
        target_tokens.reshape(grid // 2, 2, rep, own_rows), lax.axis_index("rep"), 1, 2
    )[:, :, 0]
    targets_own = lax.dynamic_slice_in_dim(targets, side, 1, 1).reshape(-1)
    targets_other = lax.dynamic_slice_in_dim(targets, 1 - side, 1, 1).reshape(-1)
    column_start = lax.axis_index("grid") * (vocab.shape[0] * vocab.shape[2])
    stats_own = row_stats(normed_own, vocab, targets_own, column_start)
    stats_other = row_stats(normed_other, vocab, targets_other, column_start)
    pieces = jnp.stack([stats_own, stats_other])
    pieces = jnp.where(side == 0, pieces, pieces[::-1]).reshape(2, 3, grid // 2, own_rows)
    pieces = pieces.transpose(2, 0, 1, 3).reshape(grid, 3 * own_rows)
    found = lax.all_to_all(pieces, "grid", 0, 0, tiled=True).reshape(grid, 3, own_rows)
    top = jnp.max(found[:, 0], axis=0)
    total = jnp.sum(found[:, 1] * jnp.exp(found[:, 0] - top[None]), axis=0)
    logprob = jnp.sum(found[:, 2], axis=0) - top - jnp.log(total)
    return (mixed, logprob)


def solution(mesh):
    in_specs = (
        P(("groups", "grid", "rep"), "row"),
        P("groups"),
        P(("row", "rep"), "grid"),
        P(("row", "rep"), "grid"),
        P("grid", ("row", "rep")),
        P("row"),
        P("row", ("grid", "rep")),
    )
    out_specs = (P(("groups", "grid", "rep"), "row"), P(("groups", "grid", "rep")))
    return jax.shard_map(
        device_step, mesh=mesh, in_specs=in_specs, out_specs=out_specs, check_vma=False
    )
```

```python
import jax
import jax.numpy as jnp
from jax import lax
from jax.sharding import PartitionSpec as P

GATE_UP_REACH = 0.09375
DOWN_REACH = 0.046875


def parity_groups(size):
    return [list(range(side, size, 2)) for side in (0, 1)]


def swapped_in_pairs(value, axis):
    size = lax.axis_size(axis)
    return lax.ppermute(value, axis, [(i, i ^ 1) for i in range(size)])


def sent_to_all(value, axis):
    peers = lax.axis_size(axis)
    return lax.all_to_all(
        jnp.broadcast_to(value[None], (peers, *value.shape)), axis, 0, 0, tiled=True
    )


def shifted(value, axis, step):
    size = lax.axis_size(axis)
    return lax.ppermute(value, axis, [(i, (i + step) % size) for i in range(size)])


def turned(blocks, axis, sign):
    size = len(blocks)
    place = lax.axis_index(axis)
    return [
        lax.select_n(place, *(blocks[(k + sign * j) % size] for j in range(size))) for k in range(size)
    ]


def both_halves(part, axis):
    return part + lax.ppermute(part, axis, [(0, 1), (1, 0)])


def summed_products(parts, weights):
    return sum(
        lax.dot_general(p, w, (((1,), (1,)), ((), ())), preferred_element_type=jnp.float32)
        for p, w in zip(parts, weights)
    )


def row_stats(normed, weights, targets, column_start):
    part = jnp.einsum("tk,rkv->rtv", normed, weights, preferred_element_type=jnp.float32)
    logits = both_halves(part, "row")
    ids = lax.broadcasted_iota(jnp.int32, logits.shape, 0) * logits.shape[2] + lax.broadcasted_iota(
        jnp.int32, logits.shape, 2
    )
    top = jnp.max(logits, axis=(0, 2))
    total = jnp.sum(jnp.exp(logits - top[None, :, None]), axis=(0, 2))
    picked = jnp.sum(
        jnp.where(ids == (targets - column_start)[None, :, None], logits, 0.0), axis=(0, 2)
    )
    return jnp.stack([top, total, picked])


def device_step(tokens, target_tokens, gate_weight, up_weight, down_weight, norm_gain, vocab_weight):
    own_rows, half_width = tokens.shape
    features = half_width * lax.axis_size("row")
    grid = lax.axis_size("grid")
    rep = lax.axis_size("rep")
    side = lax.rem(lax.axis_index("grid"), 2)

    units = down_weight.shape[0]
    block = jnp.concatenate([gate_weight.T, down_weight, up_weight.T], axis=0)
    after = shifted(block, "rep", -1)
    before = shifted(block, "rep", 1)

    own = lax.all_gather(tokens, "grid", axis=0, axis_index_groups=parity_groups(grid))
    own = own.reshape(-1, half_width)
    own, after, before = lax.optimization_barrier((own, after, before))
    middle = block.shape[0] // 2
    far_first = shifted(after[:middle], "rep", -1)
    far_last = shifted(before[middle:], "rep", 1)
    other = swapped_in_pairs(own, "grid")
    vocab = sent_to_all(vocab_weight, "rep")
    parts = [
        jnp.concatenate(pair, axis=0)
        for pair in zip(
            turned(jnp.split(other, rep, axis=1), "rep", 1), turned(jnp.split(own, rep, axis=1), "rep", 1)
        )
    ]
    length = lax.psum(sum(jnp.sum(jnp.abs(p.astype(jnp.float32)), axis=1) for p in parts), "row")
    reach = jnp.square(GATE_UP_REACH * length) * (DOWN_REACH * units * grid)
    reach = jnp.maximum(reach, 1e-20) / 30000.0
    share = (1.0 / reach)[:, None]
    half = own.shape[0]

    gate_part = summed_products(
        parts, [block[:units], after[:units], far_first[:units], before[:units]]
    )
    up_part = summed_products(
        parts,
        [block[2 * units :], after[2 * units :], far_last[2 * units - middle :], before[2 * units :]],
    )
    gate_value, up_value = both_halves(gate_part, "row"), both_halves(up_part, "row")
    hidden = (jax.nn.silu(gate_value) * up_value).astype(jnp.bfloat16)
    far_down = jnp.concatenate([far_first[units:], far_last[: 2 * units - middle]], axis=0)
    downs = [block[units : 2 * units], after[units : 2 * units], far_down, before[units : 2 * units]]
    branch = [jnp.dot(hidden, w, preferred_element_type=jnp.float32) for w in downs]
    branch_other, branch_own = (
        jnp.concatenate(turned([p[side] for p in branch], "rep", -1), axis=1) * share[side]
        for side in (slice(0, half), slice(half, 2 * half))
    )
    arrived = swapped_in_pairs(branch_other.astype(jnp.float16), "grid")
    pair_sum = (branch_own + arrived.astype(jnp.float32)).astype(jnp.float16)
    branch = lax.psum(pair_sum, "grid", axis_index_groups=parity_groups(grid))
    mixed_own = (own.astype(jnp.float32) + branch.astype(jnp.float32) * reach[half:, None]).astype(
        jnp.bfloat16
    )
    mixed = lax.dynamic_slice_in_dim(mixed_own, lax.div(lax.axis_index("grid"), 2) * own_rows, own_rows, 0)
    held = lax.optimization_barrier(mixed_own)
    held_other = swapped_in_pairs(held, "grid")
    squares = lax.psum(jnp.sum(jnp.square(held.astype(jnp.float32)), axis=1), "row")
    scale = lax.rsqrt(squares / features + 1e-05)
    scale_other = swapped_in_pairs(scale, "grid")
    normed_own, normed_other = (
        (rows.astype(jnp.float32) * factor[:, None] * norm_gain[None, :]).astype(jnp.bfloat16)
        for rows, factor in ((held, scale), (held_other, scale_other))
    )
    targets = lax.dynamic_slice_in_dim(
        target_tokens.reshape(grid // 2, 2, rep, own_rows), lax.axis_index("rep"), 1, 2
    )[:, :, 0]
    targets_own = lax.dynamic_slice_in_dim(targets, side, 1, 1).reshape(-1)
    targets_other = lax.dynamic_slice_in_dim(targets, 1 - side, 1, 1).reshape(-1)
    column_start = lax.axis_index("grid") * (vocab.shape[0] * vocab.shape[2])
    stats_own = row_stats(normed_own, vocab, targets_own, column_start)
    stats_other = row_stats(normed_other, vocab, targets_other, column_start)
    pieces = jnp.stack([stats_own, stats_other])
    pieces = jnp.where(side == 0, pieces, pieces[::-1]).reshape(2, 3, grid // 2, own_rows)
    pieces = pieces.transpose(2, 0, 1, 3).reshape(grid, 3 * own_rows)
    found = lax.all_to_all(pieces, "grid", 0, 0, tiled=True).reshape(grid, 3, own_rows)
    top = jnp.max(found[:, 0], axis=0)
    total = jnp.sum(found[:, 1] * jnp.exp(found[:, 0] - top[None]), axis=0)
    logprob = jnp.sum(found[:, 2], axis=0) - top - jnp.log(total)
    return (mixed, logprob)


def solution(mesh):
    in_specs = (
        P(("groups", "grid", "rep"), "row"),
        P("groups"),
        P(("row", "rep"), "grid"),
        P(("row", "rep"), "grid"),
        P("grid", ("row", "rep")),
        P("row"),
        P("row", ("grid", "rep")),
    )
    out_specs = (P(("groups", "grid", "rep"), "row"), P(("groups", "grid", "rep")))
    return jax.shard_map(device_step, mesh=mesh, in_specs=in_specs, out_specs=out_specs, check_vma=False)
```

```python
import jax
import jax.numpy as jnp
from jax import lax
from jax.sharding import PartitionSpec as P

GATE_UP_REACH = 0.09375
DOWN_REACH = 0.046875


def parity_groups(size):
    return [list(range(side, size, 2)) for side in (0, 1)]


def swapped_in_pairs(value, axis):
    size = lax.axis_size(axis)
    return lax.ppermute(value, axis, [(i, i ^ 1) for i in range(size)])


def sent_to_all(value, axis):
    peers = lax.axis_size(axis)
    return lax.all_to_all(
        jnp.broadcast_to(value[None], (peers, *value.shape)), axis, 0, 0, tiled=True
    )


def shifted(value, axis, step):
    size = lax.axis_size(axis)
    return lax.ppermute(value, axis, [(i, (i + step) % size) for i in range(size)])


def turned(blocks, axis, sign):
    size = len(blocks)
    place = lax.axis_index(axis)
    return [
        lax.select_n(place, *(blocks[(k + sign * j) % size] for j in range(size))) for k in range(size)
    ]


def both_halves(part, axis):
    return part + lax.ppermute(part, axis, [(0, 1), (1, 0)])


def summed_products(parts, weights):
    return sum(
        lax.dot_general(p, w, (((1,), (1,)), ((), ())), preferred_element_type=jnp.float32)
        for p, w in zip(parts, weights)
    )


def row_stats(normed, weights, targets, column_start):
    part = jnp.einsum("tk,rkv->rtv", normed, weights, preferred_element_type=jnp.float32)
    logits = both_halves(part, "row")
    ids = lax.broadcasted_iota(jnp.int32, logits.shape, 0) * logits.shape[2] + lax.broadcasted_iota(
        jnp.int32, logits.shape, 2
    )
    top = jnp.max(logits, axis=(0, 2))
    total = jnp.sum(jnp.exp(logits - top[None, :, None]), axis=(0, 2))
    picked = jnp.sum(
        jnp.where(ids == (targets - column_start)[None, :, None], logits, 0.0), axis=(0, 2)
    )
    return jnp.stack([top, total, picked])


def device_step(tokens, target_tokens, gate_weight, up_weight, down_weight, norm_gain, vocab_weight):
    own_rows, half_width = tokens.shape
    features = half_width * lax.axis_size("row")
    grid = lax.axis_size("grid")
    rep = lax.axis_size("rep")
    side = lax.rem(lax.axis_index("grid"), 2)

    units = down_weight.shape[0]
    block = jnp.concatenate([gate_weight.T, down_weight, up_weight.T], axis=0)
    after = shifted(block, "rep", -1)
    before = shifted(block, "rep", 1)

    own = lax.all_gather(tokens, "grid", axis=0, axis_index_groups=parity_groups(grid))
    own = own.reshape(-1, half_width)
    own, after, before = lax.optimization_barrier((own, after, before))
    middle = block.shape[0] // 2
    far_first = shifted(after[:middle], "rep", -1)
    far_last = shifted(before[middle:], "rep", 1)
    other = swapped_in_pairs(own, "grid")
    vocab = sent_to_all(vocab_weight, "rep")
    parts = [
        jnp.concatenate(pair, axis=0)
        for pair in zip(
            turned(jnp.split(other, rep, axis=1), "rep", 1), turned(jnp.split(own, rep, axis=1), "rep", 1)
        )
    ]
    length = lax.psum(sum(jnp.sum(jnp.abs(p.astype(jnp.float32)), axis=1) for p in parts), "row")
    reach = jnp.square(GATE_UP_REACH * length) * (DOWN_REACH * units * grid)
    reach = jnp.maximum(reach, 1e-20) / 30000.0
    half = own.shape[0]

    parts[2], reach = lax.optimization_barrier((parts[2], reach))
    share = (1.0 / reach)[:, None]
    gate_part = summed_products(
        parts, [block[:units], after[:units], far_first[:units], before[:units]]
    )
    up_part = summed_products(
        parts,
        [block[2 * units :], after[2 * units :], far_last[2 * units - middle :], before[2 * units :]],
    )
    gate_value, up_value = both_halves(gate_part, "row"), both_halves(up_part, "row")
    hidden = (jax.nn.silu(gate_value) * up_value).astype(jnp.bfloat16)
    far_down = jnp.concatenate([far_first[units:], far_last[: 2 * units - middle]], axis=0)
    downs = [block[units : 2 * units], after[units : 2 * units], far_down, before[units : 2 * units]]
    branch = [jnp.dot(hidden, w, preferred_element_type=jnp.float32) for w in downs]
    branch_other, branch_own = (
        [p * share[side] for p in turned([p[side] for p in branch], "rep", -1)]
        for side in (slice(0, half), slice(half, 2 * half))
    )
    sums = []
    for step, blocks_of in ((1, slice(0, rep // 2)), (-1, slice(rep // 2, rep))):
        leaving = jnp.concatenate(branch_other[blocks_of], axis=1).astype(jnp.float16)
        arrived = shifted(leaving, "grid", step)
        sums.append(jnp.concatenate(branch_own[blocks_of], axis=1) + arrived.astype(jnp.float32))
    pair_sum = jnp.concatenate(sums, axis=1).astype(jnp.float16)
    branch = lax.psum(pair_sum, "grid", axis_index_groups=parity_groups(grid))
    mixed_own = (own.astype(jnp.float32) + branch.astype(jnp.float32) * reach[half:, None]).astype(
        jnp.bfloat16
    )
    mixed = lax.dynamic_slice_in_dim(mixed_own, lax.div(lax.axis_index("grid"), 2) * own_rows, own_rows, 0)
    held = lax.optimization_barrier(mixed_own)
    held_other = swapped_in_pairs(held, "grid")
    squares = lax.psum(jnp.sum(jnp.square(held.astype(jnp.float32)), axis=1), "row")
    scale = lax.rsqrt(squares / features + 1e-05)
    scale_other = swapped_in_pairs(scale, "grid")
    normed_own, normed_other = (
        (rows.astype(jnp.float32) * factor[:, None] * norm_gain[None, :]).astype(jnp.bfloat16)
        for rows, factor in ((held, scale), (held_other, scale_other))
    )
    targets = lax.dynamic_slice_in_dim(
        target_tokens.reshape(grid // 2, 2, rep, own_rows), lax.axis_index("rep"), 1, 2
    )[:, :, 0]
    targets_own = lax.dynamic_slice_in_dim(targets, side, 1, 1).reshape(-1)
    targets_other = lax.dynamic_slice_in_dim(targets, 1 - side, 1, 1).reshape(-1)
    column_start = lax.axis_index("grid") * (vocab.shape[0] * vocab.shape[2])
    stats_own = row_stats(normed_own, vocab, targets_own, column_start)
    stats_other = row_stats(normed_other, vocab, targets_other, column_start)
    pieces = jnp.stack([stats_own, stats_other])
    pieces = jnp.where(side == 0, pieces, pieces[::-1]).reshape(2, 3, grid // 2, own_rows)
    pieces = pieces.transpose(2, 0, 1, 3).reshape(grid, 3 * own_rows)
    found = lax.all_to_all(pieces, "grid", 0, 0, tiled=True).reshape(grid, 3, own_rows)
    top = jnp.max(found[:, 0], axis=0)
    total = jnp.sum(found[:, 1] * jnp.exp(found[:, 0] - top[None]), axis=0)
    logprob = jnp.sum(found[:, 2], axis=0) - top - jnp.log(total)
    return (mixed, logprob)


def solution(mesh):
    in_specs = (
        P(("groups", "grid", "rep"), "row"),
        P("groups"),
        P(("row", "rep"), "grid"),
        P(("row", "rep"), "grid"),
        P("grid", ("row", "rep")),
        P("row"),
        P("row", ("grid", "rep")),
    )
    out_specs = (P(("groups", "grid", "rep"), "row"), P(("groups", "grid", "rep")))
    return jax.shard_map(device_step, mesh=mesh, in_specs=in_specs, out_specs=out_specs, check_vma=False)
```

```python
import jax
import jax.numpy as jnp
from jax import lax
from jax.sharding import PartitionSpec as P

GATE_UP_REACH = 0.09375
DOWN_REACH = 0.046875


def parity_groups(size):
    return [list(range(side, size, 2)) for side in (0, 1)]


def swapped_in_pairs(value, axis):
    size = lax.axis_size(axis)
    return lax.ppermute(value, axis, [(i, i ^ 1) for i in range(size)])


def sent_to_all(value, axis):
    peers = lax.axis_size(axis)
    return lax.all_to_all(
        jnp.broadcast_to(value[None], (peers, *value.shape)), axis, 0, 0, tiled=True
    )


def shifted(value, axis, step):
    size = lax.axis_size(axis)
    return lax.ppermute(value, axis, [(i, (i + step) % size) for i in range(size)])


def class_groups(size):
    return [list(range(side, size, 4)) for side in range(4)]


def turned(blocks, place, sign):
    size = len(blocks)
    return [
        lax.select_n(place, *(blocks[(k + sign * j) % size] for j in range(size))) for k in range(size)
    ]


def both_halves(part, axis):
    return part + lax.ppermute(part, axis, [(0, 1), (1, 0)])


def summed_products(parts, weights):
    return sum(
        lax.dot_general(p, w, (((1,), (1,)), ((), ())), preferred_element_type=jnp.float32)
        for p, w in zip(parts, weights)
    )


def row_stats(normed, weights, targets, column_start):
    part = jnp.einsum("tk,rkv->rtv", normed, weights, preferred_element_type=jnp.float32)
    logits = both_halves(part, "row")
    ids = lax.broadcasted_iota(jnp.int32, logits.shape, 0) * logits.shape[2] + lax.broadcasted_iota(
        jnp.int32, logits.shape, 2
    )
    top = jnp.max(logits, axis=(0, 2))
    total = jnp.sum(jnp.exp(logits - top[None, :, None]), axis=(0, 2))
    picked = jnp.sum(
        jnp.where(ids == (targets - column_start)[None, :, None], logits, 0.0), axis=(0, 2)
    )
    return jnp.stack([top, total, picked])


def device_step(tokens, target_tokens, gate_weight, up_weight, down_weight, norm_gain, vocab_weight):
    own_rows, half_width = tokens.shape
    features = half_width * lax.axis_size("row")
    grid = lax.axis_size("grid")
    rep = lax.axis_size("rep")
    side = lax.rem(lax.axis_index("grid"), 2)

    units = down_weight.shape[0]
    block = jnp.concatenate([gate_weight.T, down_weight, up_weight.T], axis=0)
    after = shifted(block, "rep", -1)
    before = shifted(block, "rep", 1)

    own = lax.all_gather(tokens, "grid", axis=0, axis_index_groups=parity_groups(grid))
    own = own.reshape(-1, half_width)
    own, after, before = lax.optimization_barrier((own, after, before))
    middle = block.shape[0] // 2
    far_first = shifted(after[:middle], "rep", -1)
    far_last = shifted(before[middle:], "rep", 1)
    other = swapped_in_pairs(own, "grid")
    vocab = sent_to_all(vocab_weight, "rep")
    here = lax.axis_index("grid")
    rep_place = lax.axis_index("rep")
    quad = lax.rem(here, 4)
    second = lax.div(quad, 2)

    def by_class(rows, first):
        even, odd = (
            rows.reshape(grid // 4, 2, own_rows, half_width)[:, side].reshape(-1, half_width)
            for side in (0, 1)
        )
        return jnp.where(first == 0, even, odd), jnp.where(first == 0, odd, even)

    on_0, on_2 = by_class(own, second)
    on_1, on_3 = by_class(other, lax.rem(second + side, 2))
    sets = [turned(jnp.split(rows, rep, axis=1), rep_place, 1) for rows in (on_1, on_3, on_2, on_0)]
    parts = [jnp.concatenate(pieces, axis=0) for pieces in zip(*sets)]
    length = lax.psum(sum(jnp.sum(jnp.abs(p.astype(jnp.float32)), axis=1) for p in parts), "row")
    reach = jnp.square(GATE_UP_REACH * length) * (DOWN_REACH * units * grid)
    reach = jnp.maximum(reach, 1e-20) / 30000.0
    share = (1.0 / reach)[:, None]
    count = on_0.shape[0]

    gate_part = summed_products(
        parts, [block[:units], after[:units], far_first[:units], before[:units]]
    )
    up_part = summed_products(
        parts,
        [block[2 * units :], after[2 * units :], far_last[2 * units - middle :], before[2 * units :]],
    )
    gate_value, up_value = both_halves(gate_part, "row"), both_halves(up_part, "row")
    hidden = (jax.nn.silu(gate_value) * up_value).astype(jnp.bfloat16)
    far_down = jnp.concatenate([far_first[units:], far_last[: 2 * units - middle]], axis=0)
    downs = [block[units : 2 * units], after[units : 2 * units], far_down, before[units : 2 * units]]
    branch = [jnp.dot(hidden, w, preferred_element_type=jnp.float32) for w in downs]
    to_1, to_3, to_2, kept = (
        jnp.concatenate(turned([p[rows] for p in branch], rep_place, -1), axis=1) * share[rows]
        for rows in (slice(k * count, (k + 1) * count) for k in range(4))
    )
    from_2 = shifted(to_2.astype(jnp.float16), "grid", 2)
    from_3 = shifted(to_1.astype(jnp.float16), "grid", 1)
    from_1 = shifted(to_3.astype(jnp.float16), "grid", -1)
    pair_sum = kept + from_1.astype(jnp.float32) + from_3.astype(jnp.float32)
    pair_sum = (pair_sum + from_2.astype(jnp.float32)).astype(jnp.float16)
    branch = lax.psum(pair_sum, "grid", axis_index_groups=class_groups(grid))
    mixed_own = (
        on_0.astype(jnp.float32) + branch.astype(jnp.float32) * reach[3 * count :, None]
    ).astype(jnp.bfloat16)
    mixed = lax.dynamic_slice_in_dim(mixed_own, lax.div(here, 4) * own_rows, own_rows, 0)
    held = lax.optimization_barrier(mixed_own).astype(jnp.float32)
    squares = lax.psum(jnp.sum(held * held, axis=1), "row")
    scale = lax.rsqrt(squares / features + 1e-05)
    normed = (held * scale[:, None] * norm_gain[None, :]).astype(jnp.bfloat16)
    normed_2 = shifted(normed, "grid", 2)
    normed_3 = shifted(normed, "grid", 1)
    normed_1 = shifted(normed, "grid", -1)
    others = jnp.concatenate([normed_1, normed_2, normed_3], axis=0)

    targets = lax.dynamic_slice_in_dim(
        target_tokens.reshape(grid // 4, 4, rep, own_rows), rep_place, 1, 2
    )[:, :, 0]
    targets = turned([targets[:, k].reshape(-1) for k in range(4)], quad, 1)
    column_start = here * (vocab.shape[0] * vocab.shape[2])
    stats_own = row_stats(normed, vocab, targets[0], column_start)
    stats_others = row_stats(others, vocab, jnp.concatenate(targets[1:]), column_start)
    stats = [stats_own, *jnp.split(stats_others, 3, axis=1)]
    pieces = jnp.stack([p.reshape(3, grid // 4, own_rows) for p in turned(stats, quad, -1)])
    pieces = pieces.transpose(2, 0, 1, 3).reshape(grid, 3 * own_rows)
    found = lax.all_to_all(pieces, "grid", 0, 0, tiled=True).reshape(grid, 3, own_rows)
    top = jnp.max(found[:, 0], axis=0)
    total = jnp.sum(found[:, 1] * jnp.exp(found[:, 0] - top[None]), axis=0)
    logprob = jnp.sum(found[:, 2], axis=0) - top - jnp.log(total)
    return (mixed, logprob)


def solution(mesh):
    in_specs = (
        P(("groups", "grid", "rep"), "row"),
        P("groups"),
        P(("row", "rep"), "grid"),
        P(("row", "rep"), "grid"),
        P("grid", ("row", "rep")),
        P("row"),
        P("row", ("grid", "rep")),
    )
    out_specs = (P(("groups", "grid", "rep"), "row"), P(("groups", "grid", "rep")))
    return jax.shard_map(device_step, mesh=mesh, in_specs=in_specs, out_specs=out_specs, check_vma=False)
```

```python
import jax
import jax.numpy as jnp
from jax import lax
from jax.sharding import PartitionSpec as P

GATE_UP_REACH = 0.09375
DOWN_REACH = 0.046875


def parity_groups(size):
    return [list(range(side, size, 2)) for side in (0, 1)]


def swapped_in_pairs(value, axis):
    size = lax.axis_size(axis)
    return lax.ppermute(value, axis, [(i, i ^ 1) for i in range(size)])


def sent_to_all(value, axis):
    peers = lax.axis_size(axis)
    return lax.all_to_all(
        jnp.broadcast_to(value[None], (peers, *value.shape)), axis, 0, 0, tiled=True
    )


def shifted(value, axis, step):
    size = lax.axis_size(axis)
    return lax.ppermute(value, axis, [(i, (i + step) % size) for i in range(size)])


def class_groups(size):
    return [list(range(side, size, 4)) for side in range(4)]


def halves_both_ways(value, axis, step):
    first, last = jnp.split(value, 2, axis=1)
    return shifted(first, axis, step), shifted(last, axis, -step)


def turned(blocks, place, sign):
    size = len(blocks)
    return [
        lax.select_n(place, *(blocks[(k + sign * j) % size] for j in range(size))) for k in range(size)
    ]


def both_halves(part, axis):
    return part + lax.ppermute(part, axis, [(0, 1), (1, 0)])


def summed_products(parts, weights):
    return sum(
        lax.dot_general(p, w, (((1,), (1,)), ((), ())), preferred_element_type=jnp.float32)
        for p, w in zip(parts, weights)
    )


def row_stats(normed, weights, targets, column_start):
    part = jnp.einsum("tk,rkv->rtv", normed, weights, preferred_element_type=jnp.float32)
    logits = both_halves(part, "row")
    ids = lax.broadcasted_iota(jnp.int32, logits.shape, 0) * logits.shape[2] + lax.broadcasted_iota(
        jnp.int32, logits.shape, 2
    )
    top = jnp.max(logits, axis=(0, 2))
    total = jnp.sum(jnp.exp(logits - top[None, :, None]), axis=(0, 2))
    picked = jnp.sum(
        jnp.where(ids == (targets - column_start)[None, :, None], logits, 0.0), axis=(0, 2)
    )
    return jnp.stack([top, total, picked])


def device_step(tokens, target_tokens, gate_weight, up_weight, down_weight, norm_gain, vocab_weight):
    own_rows, half_width = tokens.shape
    features = half_width * lax.axis_size("row")
    grid = lax.axis_size("grid")
    rep = lax.axis_size("rep")
    side = lax.rem(lax.axis_index("grid"), 2)

    units = down_weight.shape[0]
    block = jnp.concatenate([gate_weight.T, down_weight, up_weight.T], axis=0)
    after = shifted(block, "rep", -1)
    before = shifted(block, "rep", 1)

    own = lax.all_gather(tokens, "grid", axis=0, axis_index_groups=parity_groups(grid))
    own = own.reshape(-1, half_width)
    own, after, before = lax.optimization_barrier((own, after, before))
    middle = block.shape[0] // 2
    far_first = shifted(after[:middle], "rep", -1)
    far_last = shifted(before[middle:], "rep", 1)
    other = swapped_in_pairs(own, "grid")
    vocab = sent_to_all(vocab_weight, "rep")
    here = lax.axis_index("grid")
    rep_place = lax.axis_index("rep")
    quad = lax.rem(here, 4)
    second = lax.div(quad, 2)

    def by_class(rows, first):
        even, odd = (
            rows.reshape(grid // 4, 2, own_rows, half_width)[:, side].reshape(-1, half_width)
            for side in (0, 1)
        )
        return jnp.where(first == 0, even, odd), jnp.where(first == 0, odd, even)

    on_0, on_2 = by_class(own, second)
    on_1, on_3 = by_class(other, lax.rem(second + side, 2))
    sets = [turned(jnp.split(rows, rep, axis=1), rep_place, 1) for rows in (on_1, on_3, on_2, on_0)]
    parts = [jnp.concatenate(pieces, axis=0) for pieces in zip(*sets)]
    length = lax.psum(sum(jnp.sum(jnp.abs(p.astype(jnp.float32)), axis=1) for p in parts), "row")
    reach = jnp.square(GATE_UP_REACH * length) * (DOWN_REACH * units * grid)
    reach = jnp.maximum(reach, 1e-20) / 30000.0
    share = (1.0 / reach)[:, None]
    count = on_0.shape[0]

    gate_part = summed_products(
        parts, [block[:units], after[:units], far_first[:units], before[:units]]
    )
    up_part = summed_products(
        parts,
        [block[2 * units :], after[2 * units :], far_last[2 * units - middle :], before[2 * units :]],
    )
    gate_value, up_value = both_halves(gate_part, "row"), both_halves(up_part, "row")
    hidden = (jax.nn.silu(gate_value) * up_value).astype(jnp.bfloat16)
    far_down = jnp.concatenate([far_first[units:], far_last[: 2 * units - middle]], axis=0)
    downs = [block[units : 2 * units], after[units : 2 * units], far_down, before[units : 2 * units]]
    branch = [jnp.dot(hidden, w, preferred_element_type=jnp.float32) for w in downs]
    to_1, to_3, to_2, kept = (
        jnp.concatenate(turned([p[rows] for p in branch], rep_place, -1), axis=1) * share[rows]
        for rows in (slice(k * count, (k + 1) * count) for k in range(4))
    )
    from_2 = halves_both_ways(to_2.astype(jnp.float16), "grid", 2)
    from_3 = shifted(to_1.astype(jnp.float16), "grid", 1)
    from_1 = shifted(to_3.astype(jnp.float16), "grid", -1)
    pair_sum = kept + from_1.astype(jnp.float32) + from_3.astype(jnp.float32)
    pair_sum = (pair_sum + jnp.concatenate(from_2, axis=1).astype(jnp.float32)).astype(jnp.float16)
    branch = lax.psum(pair_sum, "grid", axis_index_groups=class_groups(grid))
    mixed_own = (
        on_0.astype(jnp.float32) + branch.astype(jnp.float32) * reach[3 * count :, None]
    ).astype(jnp.bfloat16)
    mixed = lax.dynamic_slice_in_dim(mixed_own, lax.div(here, 4) * own_rows, own_rows, 0)
    held = lax.optimization_barrier(mixed_own).astype(jnp.float32)
    squares = lax.psum(jnp.sum(held * held, axis=1), "row")
    scale = lax.rsqrt(squares / features + 1e-05)
    normed = (held * scale[:, None] * norm_gain[None, :]).astype(jnp.bfloat16)
    normed_2 = halves_both_ways(normed, "grid", 2)
    normed_3 = shifted(normed, "grid", 1)
    normed_1 = shifted(normed, "grid", -1)
    others = jnp.concatenate([normed_1, jnp.concatenate(normed_2, axis=1), normed_3], axis=0)

    targets = lax.dynamic_slice_in_dim(
        target_tokens.reshape(grid // 4, 4, rep, own_rows), rep_place, 1, 2
    )[:, :, 0]
    targets = turned([targets[:, k].reshape(-1) for k in range(4)], quad, 1)
    column_start = here * (vocab.shape[0] * vocab.shape[2])
    stats_own = row_stats(normed, vocab, targets[0], column_start)
    stats_others = row_stats(others, vocab, jnp.concatenate(targets[1:]), column_start)
    stats = [stats_own, *jnp.split(stats_others, 3, axis=1)]
    pieces = jnp.stack([p.reshape(3, grid // 4, own_rows) for p in turned(stats, quad, -1)])
    pieces = pieces.transpose(2, 0, 1, 3).reshape(grid, 3 * own_rows)
    found = lax.all_to_all(pieces, "grid", 0, 0, tiled=True).reshape(grid, 3, own_rows)
    top = jnp.max(found[:, 0], axis=0)
    total = jnp.sum(found[:, 1] * jnp.exp(found[:, 0] - top[None]), axis=0)
    logprob = jnp.sum(found[:, 2], axis=0) - top - jnp.log(total)
    return (mixed, logprob)


def solution(mesh):
    in_specs = (
        P(("groups", "grid", "rep"), "row"),
        P("groups"),
        P(("row", "rep"), "grid"),
        P(("row", "rep"), "grid"),
        P("grid", ("row", "rep")),
        P("row"),
        P("row", ("grid", "rep")),
    )
    out_specs = (P(("groups", "grid", "rep"), "row"), P(("groups", "grid", "rep")))
    return jax.shard_map(device_step, mesh=mesh, in_specs=in_specs, out_specs=out_specs, check_vma=False)
```
